32 devices in a mesh: rows: 8 (over z, x), cols: 4 (over y, core).
Axes of the slice: x: 2, y: 2, z: 4, core: 2. Of those that a mesh axis runs over, the one named last changes fastest.
Arguments:
- rhs: float32 [2, 4096, 512], P(None, 'rows', 'cols'), may hold values from -6 to 6
- diag_blocks: float32 [2, 512, 512], replicated, may hold values from -0.25 to 0.25
- multipliers: float32 [2, 2, 4096, 512], P(None, None, 'rows'), may hold values from -0.25 to 0.25
- pivots: int32 [1024], P('cols'), may hold values from 0 to 8191, as said below
Outputs:
- solved: float32 [2, 4096, 512], P(None, 'rows', 'cols')
The draws below stay inside these ranges and needn't reach their ends.
Inputs may be any that keep to these rules, and one draw needn't show every extreme that they name: pivots[i] is i or a row at 1024 or beyond; the rows at 1024 or beyond that pivots names are all different, and at most 192 of them lie among the rows held by one index of rows, a number that some index reaches.
All inputs are finite; a program needn't handle non-finite values.
Results may differ from the reference program's by a relative error of at most 0.0001.
Values sent between devices are 32-bit elements; how exact they have to be, the bound alone decides.
A program may use at most 64 MiB of HBM per device.

```python
import jax
import jax.numpy as jnp
from jax import lax

BLK = 512
PANELS = 2
CYC = 2
R = 512
PB = 1024
MOVE = 192
N_ROWS = 8


def draw_pivots(key, part):
    key_owner, key_slot, key_keep, key_row = jax.random.split(jax.random.fold_in(key, 17), 4)
    places = jnp.arange(PB, dtype=jnp.int32)
    local = CYC * BLK
    chosen = jax.random.randint(key_owner, (), 0, N_ROWS, dtype=jnp.int32)
    slot_count = N_ROWS * MOVE
    slot_ids = jnp.arange(slot_count, dtype=jnp.int32)
    slot_owner = slot_ids // MOVE
    slot_score = jax.random.randint(key_slot, (slot_count,), 0, 32768, dtype=jnp.int32) * slot_count + slot_ids
    slot_score = jnp.where(slot_owner == chosen, 1073741824 + slot_ids, slot_score)
    slot_order = jnp.argsort(slot_score).astype(jnp.int32)
    later = jnp.clip(places - MOVE, 0, slot_count - 1)
    owner = jnp.where(places < MOVE, chosen, slot_owner[slot_order[later]])
    keep = jax.random.randint(key_keep, (PB,), 0, 8, dtype=jnp.int32)
    swapped = (places < MOVE) | (keep != 0)
    owner_ids = jnp.arange(N_ROWS, dtype=jnp.int32)
    hits = ((owner[:, None] == owner_ids[None, :]) & swapped[:, None]).astype(jnp.int32)
    before = jnp.cumsum(hits, axis=0) - hits
    rank = jnp.sum(before * hits, axis=1)
    local_ids = jnp.arange(local, dtype=jnp.int32)
    row_score = jax.random.randint(key_row, (N_ROWS, local), 0, 32768, dtype=jnp.int32) * local + local_ids[None, :]
    barred = (owner_ids[:, None] < PANELS) & (local_ids[None, :] < BLK)
    row_score = jnp.where(barred, 1073741824 + local_ids[None, :], row_score)
    ranked = jnp.argsort(row_score, axis=1).astype(jnp.int32)
    local_row = ranked[owner, jnp.minimum(rank, local - 1)]
    target = local_row // BLK * (N_ROWS * BLK) + owner * BLK + local_row % BLK
    return jnp.where(swapped, target, places).astype(jnp.int32)


def shard_levels(key, dims, shards, smallest, top_value):
    def one(axis_at, parts):
        steps = jax.random.uniform(jax.random.fold_in(jax.random.fold_in(key, 6), axis_at), (parts,), jnp.float32, smallest / len(shards), top_value / len(shards))
        return jnp.repeat(jnp.exp(steps), dims[axis_at] // parts).reshape((-1,) + (1,) * (len(dims) - axis_at - 1))

    gain = one(*shards[0])
    for cut in shards[1:]:
        gain = gain * one(*cut)
    return gain


def normal_values(stream_key, dims, scale, bound, shards=(), held_as=jnp.bfloat16):
    drawn = scale * jax.random.normal(stream_key, dims, jnp.float32)
    if shards:
        drawn = drawn * shard_levels(stream_key, dims, shards, -0.22, 0.18)
    return jnp.clip(drawn, -bound, bound).astype(held_as)


def setup_inputs(seed: int = 0) -> dict:
    arg_keys = jax.random.split(jax.random.key(seed), 5)
    rhs = normal_values(arg_keys[0], (CYC, N_ROWS * BLK, R), 1.0, 6.0, ((1, 8), (2, 4)), jnp.float32)
    diag_blocks = normal_values(arg_keys[1], (PANELS, BLK, BLK), BLK ** -0.5, 0.25, (), jnp.float32)
    multipliers = normal_values(arg_keys[2], (PANELS, CYC, N_ROWS * BLK, BLK), BLK ** -0.5, 0.25, ((2, 8),), jnp.float32)
    pivots = draw_pivots(jax.random.fold_in(arg_keys[4], 71), 0)
    return dict(rhs=rhs, diag_blocks=diag_blocks, multipliers=multipliers, pivots=pivots)


def unit_lower_solve(factor, values):
    return lax.linalg.triangular_solve(factor, values, left_side=True, lower=True, unit_diagonal=True)

def reference(rhs, diag_blocks, multipliers, pivots):
    span = rhs.shape[1]
    width = rhs.shape[2]
    blk = diag_blocks.shape[1]
    total = rhs.shape[0] * span
    whole = rhs.reshape(total, width)

    def interchange(i, order):
        target = pivots[i]
        first = order[i]
        second = order[target]
        return order.at[i].set(second).at[target].set(first)
    order = lax.fori_loop(0, pivots.shape[0], interchange, jnp.arange(total, dtype=jnp.int32))
    permuted = whole[order]
    lower = multipliers.reshape(multipliers.shape[0], total, blk)
    for k in range(multipliers.shape[0]):
        start = k * blk
        finish = start + blk
        panel_rows = unit_lower_solve(diag_blocks[k], permuted[start:finish])
        remain = permuted[finish:] - jnp.dot(lower[k, finish:].astype(jnp.float32), panel_rows.astype(jnp.float32), precision=lax.Precision.HIGHEST, preferred_element_type=jnp.float32)
        permuted = jnp.concatenate([permuted[:start], panel_rows, remain], axis=0)
    return permuted.reshape(rhs.shape)
```

```python
import functools

import jax
import jax.numpy as jnp
from jax import lax
from jax.experimental import pallas as pl
from jax.experimental.pallas import tpu as pltpu
from jax.sharding import PartitionSpec as P

MESH = pl.DeviceIdType.MESH
F32, BF16 = jnp.float32, jnp.bfloat16


def split(x):
    hi = x.astype(BF16)
    return hi, (x - hi.astype(F32)).astype(BF16)


def mm(a, b):
    return jnp.dot(a, b, preferred_element_type=F32)


def dot3(a, b):
    (ah, al), (bh, bl) = a, b
    return mm(ah, bh) + (mm(ah, bl) + mm(al, bh))


def wide(x):
    return jnp.concatenate(split(x), axis=1)


def fold(x):
    half = x.shape[1] // 2
    return x[:, :half] + x[:, half:]


def dot_wide(a, b):
    hi, lo = split(b)
    return fold(mm(a[0], jnp.concatenate([hi, lo], axis=1))) + mm(a[1], hi)


def select_rows(onehot, x):
    return fold(mm(onehot, wide(x)))


def iota(shape, dim):
    return lax.broadcasted_iota(jnp.int32, shape, dim)


def kernel(
    ranks, groups, blk, slots, chunks,
    rhs, diag_hbm, mult_hbm, piv, out,
    panels, lbuf, comp, pivs, diag, mult, inv, mhi, mlo,
    local_sem, piv_s, piv_r, pan_up, pan_ac, pan_r, l_up, l_ac, l_r, lc_s, lc_r,
    c_up, c_dn, c_ac, c_r,
):
    m, c = lax.axis_index("rows"), lax.axis_index("cols")
    steps = ranks // 2
    j, p = m // 2, m % 2
    local_count, columns = rhs.shape
    count = 2 * blk
    hb = blk // 2
    across = m + 1 - 2 * p
    has_up, has_dn = j < steps - 1, j > 0
    up = lax.rem(m + 2, ranks)
    dn = lax.rem(m + ranks - 2, ranks)
    pending = []

    copies = [
        pltpu.make_async_copy(mult_hbm.at[0], mult.at[0], local_sem.at[0]),
        pltpu.make_async_copy(diag_hbm, diag, local_sem.at[1]),
        pltpu.make_async_copy(mult_hbm.at[1], mult.at[1], local_sem.at[2]),
    ]
    for copy in copies:
        copy.start()

    barrier = pltpu.get_barrier_semaphore()

    def greet(**where):
        pl.semaphore_signal(barrier, inc=1, device_id=where, device_id_type=MESH)

    for d in range(1, groups):
        greet(cols=lax.rem(c + d, groups))
    greet(rows=across)

    @pl.when(has_up)
    def _():
        greet(rows=up)

    @pl.when(has_dn)
    def _():
        greet(rows=dn)

    met = groups + jnp.where(has_up, 1, 0) + jnp.where(has_dn, 1, 0)
    pl.semaphore_wait(barrier, met)

    def when(cond, action):
        if cond is None:
            action()
        else:
            pl.when(cond)(action)

    def remote(src, dst, ss, rs, **where):
        return pltpu.make_async_remote_copy(
            src_ref=src, dst_ref=dst, send_sem=ss, recv_sem=rs,
            device_id=where, device_id_type=MESH,
        )

    def send(cond, *args, **where):
        copy = remote(*args, **where)
        when(cond, copy.start)
        pending.append((cond, copy))

    for d in range(1, groups):
        send(None, piv, pivs.at[c], piv_s.at[d - 1], piv_r.at[c], cols=lax.rem(c + d, groups))

    rows_per = blk // chunks

    def chunk(q):
        return pl.ds(q * rows_per, rows_per)

    for q in range(chunks):
        dst = panels.at[p, chunk(q)]
        sem = pan_r.at[p * chunks + q]
        send(j == 0, rhs.at[chunk(q)], dst, pan_up.at[q], sem, rows=up)
        send(j == 0, rhs.at[chunk(q)], dst, pan_ac.at[q], sem, rows=across)

    qr = blk // groups
    hr = qr // 2

    def lpart(h):
        return pl.ds(pl.multiple_of(c * qr + h * hr, 8), hr)

    copies[0].wait()
    send(m == 1, mult.at[0, lpart(0)], lbuf.at[lpart(0)], l_up.at[0], l_r.at[0], rows=up)
    for h in (1, 0):
        send(m == 1, mult.at[0, lpart(h)], lbuf.at[lpart(h)], l_ac.at[h], l_r.at[h], rows=across)

    @pl.when(j == 0)
    def _():
        panels[p] = rhs[:blk]

    @pl.when(m == 1)
    def _():
        lbuf[...] = mult[0, :blk]

    pivs[c] = piv[...]
    copies[1].wait()

    r_at, c_at = iota((hb, hb), 0), iota((hb, hb), 1)

    def offdiag(b, k, h):
        pair = (r_at // (2 * b) == c_at // (2 * b)) & (r_at % (2 * b) >= b) & (c_at % (2 * b) < b)
        return jnp.where(pair, diag[k, h * hb:(h + 1) * hb, h * hb:(h + 1) * hb], 0.0)

    def level(b):
        for k in range(2):
            for h in range(2):
                at = 2 * k + h
                f = offdiag(b, k, h)
                if b == 1:
                    inv[at] = jnp.where(r_at == c_at, 1.0, 0.0) - f
                else:
                    x = inv[at]
                    xs = split(x)
                    inv[at] = x - dot3(split(dot3(xs, split(f))), xs)

    def levels(lo, hi):
        b = lo
        while b < hi:
            level(b)
            b *= 2

    for d in range(1, groups):
        src = lax.rem(c + d, groups)
        remote(piv, pivs.at[src], piv_s.at[d - 1], piv_r.at[src], cols=src).wait_recv()
    pr = piv.shape[0]
    listed = pivs[...].reshape(groups * pr, 128)
    shift = blk.bit_length() - 1
    rshift = ranks.bit_length() - 1
    fresh = listed >= count
    owner = jnp.where(fresh, (listed >> shift) & (ranks - 1), -1)
    place = ((listed >> (shift + rshift)) << shift) | (listed & (blk - 1))
    ownf, placef = owner.astype(F32), place.astype(F32)

    def column(x):
        xt = x.T
        return jnp.concatenate([xt[:, k:k + 1] for k in range(groups * pr)], axis=0)

    def flat_row(x):
        return jnp.concatenate([x[k:k + 1] for k in range(groups * pr)], axis=1)

    own_col, place_col = column(ownf), column(placef)
    lanes = -(-ranks // 128) * 128
    own_hot = own_col == iota((count, lanes), 1).astype(F32)
    before = (iota((count, count), 0) > iota((count, count), 1)).astype(F32).astype(BF16)
    tally = mm(before, own_hot.astype(F32).astype(BF16))
    slot_col = jnp.sum(jnp.where(own_hot, tally, 0.0), axis=1, keepdims=True)
    mf = m.astype(F32)
    wide_slots = -(-slots // 128) * 128
    taken = (slot_col == iota((count, wide_slots), 1).astype(F32)) & (own_col == mf)
    src_row = jnp.sum(jnp.where(taken, place_col + 1.0, 0.0), axis=0, keepdims=True) - 1.0
    src_col = jnp.broadcast_to(src_row, (8, wide_slots)).T[:slots, :1]
    pick = (src_col == iota((slots, local_count), 1).astype(F32)).astype(F32).astype(BF16)

    def slab(r):
        return pl.ds(pl.multiple_of(r * slots, 8), slots)

    comp[slab(m)] = select_rows(pick, rhs[...])

    def pass_on(r, go_up, go_dn, go_ac):
        for cond, sem, to in ((go_up, c_up, up), (go_dn, c_dn, dn), (go_ac, c_ac, across)):
            if cond is not False:
                send(cond, comp.at[slab(r)], comp.at[slab(r)], sem.at[r], c_r.at[r], rows=to)

    def arrived(cond, dst, sem):
        when(cond, remote(dst, dst, l_up.at[0], sem, rows=across).wait_recv)

    pass_on(m, has_up, has_dn, None)
    levels(1, 4)

    for q in range(chunks):
        here = panels.at[p, chunk(q)]
        sem = pan_r.at[p * chunks + q]
        arrived(has_dn, here, sem)
        send(has_dn & has_up, here, here, pan_up.at[q], sem, rows=up)
        send(has_dn, here, here, pan_ac.at[q], sem, rows=across)
    mine_half = 1 - p
    here = lbuf.at[lpart(mine_half)]
    arrived(m != 1, here, l_r.at[mine_half])
    send((m != 1) & has_up, here, here, l_up.at[0], l_r.at[mine_half], rows=up)
    send(has_dn, here, here, l_ac.at[mine_half], l_r.at[mine_half], rows=across)

    def share(h):
        for d in range(1, groups):
            to = lax.rem(c + d, groups)
            part = lbuf.at[lpart(h)]
            send(m != 1, part, part, lc_s.at[h * (groups - 1) + d - 1], lc_r.at[c * 2 + h], cols=to)

    share(mine_half)

    span = hb // 4
    b = 4
    for s in range(1, steps):
        below, above = lax.rem(m - 2 * s + ranks, ranks), lax.rem(m + 2 * s, ranks)
        from_below, from_above = j >= s, j + s < steps
        arrived(from_below, comp.at[slab(below)], c_r.at[below])
        pass_on(below, from_below & has_up, False, from_below)
        arrived(from_above, comp.at[slab(above)], c_r.at[above])
        pass_on(above, False, from_above & has_dn, from_above)
        if b < hb:
            levels(b, b * 4 if s < steps - 1 else hb)
            b = b * 4
    levels(b, hb)

    other_half = p
    arrived(m != 1, lbuf.at[lpart(other_half)], l_r.at[other_half])
    share(other_half)

    copies[2].wait()
    mhi[...], mlo[...] = split(mult[...])

    for q in range(chunks):
        arrived(None, panels.at[1 - p, chunk(q)], pan_r.at[(1 - p) * chunks + q])

    to_here = jnp.where(owner == m, place, -1).astype(F32)
    to_row = flat_row(to_here)
    landing = (iota((local_count, count), 0).astype(F32) == to_row).astype(F32)
    hit = jnp.sum(landing, axis=1, keepdims=True) > 0.0
    moved_in = select_rows(landing.astype(BF16), panels[...].reshape(count, columns))
    out[...] = jnp.where(hit, moved_in, rhs[...])

    for s in range(steps):
        r = 2 * s + 1 - p
        arrived(None, comp.at[slab(r)], c_r.at[r])

    where_col = jnp.where(own_col >= 0.0, own_col * slots + slot_col, -1.0)
    pool = wide(comp[...])

    def panel_rows(k):
        target = where_col[k * blk:(k + 1) * blk]
        pick = (target == iota((blk, ranks * slots), 1).astype(F32)).astype(F32).astype(BF16)
        return jnp.where(target >= 0.0, fold(mm(pick, pool)), panels[k])

    def solve(k, values):
        first = dot_wide(split(inv[2 * k]), values[:hb])
        rest = values[hb:] - dot_wide(split(diag[k, hb:, :hb]), first)
        return jnp.concatenate([first, dot_wide(split(inv[2 * k + 1]), rest)], axis=0)

    y0 = solve(0, panel_rows(0))
    start = panel_rows(1)

    def gather_lower(h):
        for d in range(1, groups):
            src = lax.rem(c + d, groups)
            part = lbuf.at[pl.ds(pl.multiple_of(src * qr + h * hr, 8), hr)]
            arrived(m != 1, part, lc_r.at[src * 2 + h])

    gather_lower(0)
    gather_lower(1)
    y1 = solve(1, start - dot_wide(split(lbuf[...]), y0))
    out[...] = out[...] - dot_wide((mhi[0], mlo[0]), y0) - dot_wide((mhi[1], mlo[1]), y1)

    @pl.when(m == 0)
    def _():
        out[:blk] = y0

    @pl.when(m == 1)
    def _():
        out[:blk] = y1

    for cond, copy in pending:
        when(cond, copy.wait_send)


def shards(ranks, groups, rhs, diag_blocks, multipliers, pivots):
    cycles, blk, columns = rhs.shape
    local_count = cycles * blk
    count = pivots.shape[0] * groups
    slots = 3 * count // (2 * ranks)
    chunks = 4
    dma = pltpu.SemaphoreType.DMA
    solved = pl.pallas_call(
        functools.partial(kernel, ranks, groups, blk, slots, chunks),
        out_shape=jax.ShapeDtypeStruct((local_count, columns), F32),
        in_specs=[
            pl.BlockSpec(memory_space=pltpu.VMEM),
            pl.BlockSpec(memory_space=pl.ANY),
            pl.BlockSpec(memory_space=pl.ANY),
            pl.BlockSpec(memory_space=pltpu.VMEM),
        ],
        out_specs=pl.BlockSpec(memory_space=pltpu.VMEM),
        scratch_shapes=[
            pltpu.VMEM((2, blk, columns), F32),
            pltpu.VMEM((blk, blk), F32),
            pltpu.VMEM((ranks * slots, columns), F32),
            pltpu.VMEM((groups, pivots.shape[0] // 128, 128), jnp.int32),
            pltpu.VMEM((2, blk, blk), F32),
            pltpu.VMEM((2, local_count, blk), F32),
            pltpu.VMEM((4, blk // 2, blk // 2), F32),
            pltpu.VMEM((2, local_count, blk), BF16),
            pltpu.VMEM((2, local_count, blk), BF16),
            dma((3,)), dma((groups,)), dma((groups,)),
            dma((chunks,)), dma((chunks,)), dma((2 * chunks,)),
            dma((1,)), dma((2,)), dma((2,)),
            dma((2 * groups,)), dma((2 * groups,)),
            dma((ranks,)), dma((ranks,)), dma((ranks,)), dma((ranks,)),
        ],
        compiler_params=pltpu.CompilerParams(
            collective_id=0, has_side_effects=True, vmem_limit_bytes=60 * 1024 * 1024
        ),
    )(
        rhs.reshape(local_count, columns),
        diag_blocks,
        multipliers.reshape(multipliers.shape[0], local_count, blk),
        pivots.reshape(-1, 128),
    )
    return solved.reshape(cycles, blk, columns)


def solution(mesh):
    placed = (P(None, "rows", "cols"), P(), P(None, None, "rows", None), P("cols"))
    return jax.shard_map(
        functools.partial(shards, mesh.shape["rows"], mesh.shape["cols"]),
        mesh=mesh, in_specs=placed, out_specs=P(None, "rows", "cols"), check_vma=False,
    )
```

```python
import functools

import jax
import jax.numpy as jnp
from jax import lax
from jax.experimental import pallas as pl
from jax.experimental.pallas import tpu as pltpu
from jax.sharding import PartitionSpec as P

MESH = pl.DeviceIdType.MESH
F32, BF16 = jnp.float32, jnp.bfloat16


def split(x):
    hi = x.astype(BF16)
    return hi, (x - hi.astype(F32)).astype(BF16)


def mm(a, b):
    return jnp.dot(a, b, preferred_element_type=F32)


def dot3(a, b):
    (ah, al), (bh, bl) = a, b
    return mm(ah, bh) + (mm(ah, bl) + mm(al, bh))


def wide(x):
    return jnp.concatenate(split(x), axis=1)


def fold(x):
    half = x.shape[1] // 2
    return x[:, :half] + x[:, half:]


def dot_wide(a, b):
    hi, lo = split(b)
    return fold(mm(a[0], jnp.concatenate([hi, lo], axis=1))) + mm(a[1], hi)


def select_rows(onehot, x):
    return fold(mm(onehot, wide(x)))


def iota(shape, dim):
    return lax.broadcasted_iota(jnp.int32, shape, dim)


def kernel(
    ranks, groups, blk, slots, chunks, parts,
    rhs, diag_hbm, mult_hbm, piv, out,
    panels, lbuf, comp, pivs, diag, mult, inv, mhi, mlo,
    local_sem, piv_s, piv_r, pan_up, pan_ac, pan_r, l_up, l_ac, l_r, lc_s, lc_f, lc_r,
    c_up, c_dn, c_ac, c_r,
):
    m, c = lax.axis_index("rows"), lax.axis_index("cols")
    steps = ranks // 2
    j, p = m // 2, m % 2
    local_count, columns = rhs.shape
    count = 2 * blk
    hb = blk // 2
    across = m + 1 - 2 * p
    has_up, has_dn = j < steps - 1, j > 0
    up = lax.rem(m + 2, ranks)
    dn = lax.rem(m + ranks - 2, ranks)
    pending = []

    copies = [
        pltpu.make_async_copy(mult_hbm.at[0], mult.at[0], local_sem.at[0]),
        pltpu.make_async_copy(diag_hbm, diag, local_sem.at[1]),
        pltpu.make_async_copy(mult_hbm.at[1], mult.at[1], local_sem.at[2]),
    ]
    for copy in copies:
        copy.start()

    barrier = pltpu.get_barrier_semaphore()

    def greet(**where):
        pl.semaphore_signal(barrier, inc=1, device_id=where, device_id_type=MESH)

    for d in range(1, groups):
        greet(cols=lax.rem(c + d, groups))
    greet(rows=across)

    @pl.when(has_up)
    def _():
        greet(rows=up)

    @pl.when(has_dn)
    def _():
        greet(rows=dn)

    met = groups + jnp.where(has_up, 1, 0) + jnp.where(has_dn, 1, 0)
    pl.semaphore_wait(barrier, met)

    def when(cond, action):
        if cond is None:
            action()
        else:
            pl.when(cond)(action)

    def remote(src, dst, ss, rs, **where):
        return pltpu.make_async_remote_copy(
            src_ref=src, dst_ref=dst, send_sem=ss, recv_sem=rs,
            device_id=where, device_id_type=MESH,
        )

    def send(cond, *args, **where):
        copy = remote(*args, **where)
        when(cond, copy.start)
        pending.append((cond, copy))

    for d in range(1, groups):
        send(None, piv, pivs.at[c], piv_s.at[d - 1], piv_r.at[c], cols=lax.rem(c + d, groups))

    rows_per = blk // chunks

    def chunk(q):
        return pl.ds(q * rows_per, rows_per)

    qr = blk // groups
    hr = qr // 2 // chunks

    def lpart(h, q, owner=c):
        return lbuf.at[pl.ds(pl.multiple_of(owner * qr + (h * chunks + q) * hr, 8), hr)]

    def lsource(h, q):
        return mult.at[0, pl.ds(pl.multiple_of(c * qr + (h * chunks + q) * hr, 8), hr)]

    def lsem(h, q):
        return l_r.at[h * chunks + q]

    def panel_source(q):
        dst = panels.at[p, chunk(q)]
        sem = pan_r.at[p * chunks + q]
        send(j == 0, rhs.at[chunk(q)], dst, pan_up.at[q], sem, rows=up)
        send(j == 0, rhs.at[chunk(q)], dst, pan_ac.at[q], sem, rows=across)

    copies[0].wait()
    for q in range(chunks):
        send(m == 1, lsource(1, q), lpart(1, q), l_ac.at[chunks + q], lsem(1, q), rows=across)
    for q in range(chunks):
        send(m == 1, lsource(0, q), lpart(0, q), l_up.at[q], lsem(0, q), rows=up)
        send(m == 1, lsource(0, q), lpart(0, q), l_ac.at[q], lsem(0, q), rows=across)
        panel_source(q)

    @pl.when(j == 0)
    def _():
        panels[p] = rhs[:blk]

    @pl.when(m == 1)
    def _():
        lbuf[...] = mult[0, :blk]

    pivs[c] = piv[...]
    copies[1].wait()

    r_at, c_at = iota((hb, hb), 0), iota((hb, hb), 1)

    def offdiag(b, k, h):
        pair = (r_at // (2 * b) == c_at // (2 * b)) & (r_at % (2 * b) >= b) & (c_at % (2 * b) < b)
        return jnp.where(pair, diag[k, h * hb:(h + 1) * hb, h * hb:(h + 1) * hb], 0.0)

    def level(b):
        for k in range(2):
            for h in range(2):
                at = 2 * k + h
                f = offdiag(b, k, h)
                if b == 1:
                    inv[at] = jnp.where(r_at == c_at, 1.0, 0.0) - f
                else:
                    x = inv[at]
                    xs = split(x)
                    inv[at] = x - dot3(split(dot3(xs, split(f))), xs)

    def levels(lo, hi):
        b = lo
        while b < hi:
            level(b)
            b *= 2

    mine_half = 1 - p
    side = c + 1 - 2 * (c % 2)
    far = lax.rem(c + 2, groups)
    corner = groups - 1 - c

    def share(h, q, cond):
        part, at = lpart(h, q), h * chunks + q
        for n, to in enumerate((far, side)):
            send(cond, part, part, lc_s.at[n * 2 * chunks + at], lc_r.at[c * 2 * chunks + at], cols=to)

    def relay(q, cond):
        here = lpart(mine_half, q)
        arrived(cond & (m != 1), here, lsem(mine_half, q))
        send(cond & (m != 1) & has_up, here, here, l_up.at[q], lsem(mine_half, q), rows=up)
        send(cond & has_dn, here, here, l_ac.at[mine_half * chunks + q], lsem(mine_half, q), rows=across)
        share(mine_half, q, cond & (m != 1))
        here = panels.at[p, chunk(q)]
        sem = pan_r.at[p * chunks + q]
        arrived(cond & has_dn, here, sem)
        send(cond & has_dn & has_up, here, here, pan_up.at[q], sem, rows=up)
        send(cond & has_dn, here, here, pan_ac.at[q], sem, rows=across)

    def arrived(cond, dst, sem):
        when(cond, remote(dst, dst, l_up.at[0], sem, rows=across).wait_recv)

    early = j <= 1

    for d in range(1, groups):
        src = lax.rem(c + d, groups)
        remote(piv, pivs.at[src], piv_s.at[d - 1], piv_r.at[src], cols=src).wait_recv()
    pr = piv.shape[0]
    listed = pivs[...].reshape(groups * pr, 128)
    shift = blk.bit_length() - 1
    rshift = ranks.bit_length() - 1
    fresh = listed >= count
    owner = jnp.where(fresh, (listed >> shift) & (ranks - 1), -1)
    place = ((listed >> (shift + rshift)) << shift) | (listed & (blk - 1))
    ownf, placef = owner.astype(F32), place.astype(F32)

    def column(x):
        xt = x.T
        return jnp.concatenate([xt[:, k:k + 1] for k in range(groups * pr)], axis=0)

    def flat_row(x):
        return jnp.concatenate([x[k:k + 1] for k in range(groups * pr)], axis=1)

    relay(0, early)
    own_col, place_col = column(ownf), column(placef)
    lanes = -(-ranks // 128) * 128
    own_hot = own_col == iota((count, lanes), 1).astype(F32)
    before = (iota((count, count), 0) > iota((count, count), 1)).astype(F32).astype(BF16)
    tally = mm(before, own_hot.astype(F32).astype(BF16))
    slot_col = jnp.sum(jnp.where(own_hot, tally, 0.0), axis=1, keepdims=True)
    mf = m.astype(F32)
    wide_slots = -(-slots // 128) * 128
    taken = (slot_col == iota((count, wide_slots), 1).astype(F32)) & (own_col == mf)
    src_row = jnp.sum(jnp.where(taken, place_col + 1.0, 0.0), axis=0, keepdims=True) - 1.0
    src_col = jnp.broadcast_to(src_row, (8, wide_slots)).T[:slots, :1]
    pick = (src_col == iota((slots, local_count), 1).astype(F32)).astype(F32).astype(BF16)

    def slab(r):
        return pl.ds(pl.multiple_of(r * slots, 8), slots)

    part_rows = slots // parts

    def slice_of(r, n):
        return comp.at[pl.ds(pl.multiple_of(r * slots + n * part_rows, 8), part_rows)]

    comp[slab(m)] = select_rows(pick, rhs[...])

    def pass_on(r, n, go_up, go_dn, go_ac):
        here, at = slice_of(r, n), r * parts + n
        for cond, sem, to in ((go_up, c_up, up), (go_dn, c_dn, dn), (go_ac, c_ac, across)):
            if cond is not False:
                send(cond, here, here, sem.at[at], c_r.at[at], rows=to)

    for n in range(parts):
        pass_on(m, n, has_up, has_dn, None)

    relay(0, jnp.logical_not(early))
    levels(1, 4)

    b = 4
    ready = 1
    for s in range(1, steps):
        for q in range(ready, min(ready + 2, chunks)):
            relay(q, j >= 0)
        ready = min(ready + 2, chunks)
        below, above = lax.rem(m - 2 * s + ranks, ranks), lax.rem(m + 2 * s, ranks)
        from_below, from_above = j >= s, j + s < steps
        for n in range(parts):
            arrived(from_above, slice_of(above, n), c_r.at[above * parts + n])
            pass_on(above, n, False, from_above & has_dn, from_above)
        for n in range(parts):
            arrived(from_below, slice_of(below, n), c_r.at[below * parts + n])
            pass_on(below, n, from_below & has_up, False, from_below)
        if b < hb:
            levels(b, b * 4 if s < steps - 1 else hb)
            b = b * 4
    levels(b, hb)

    other_half = p
    for q in range(chunks):
        arrived(m != 1, lpart(other_half, q), lsem(other_half, q))
        share(other_half, q, m != 1)

    copies[2].wait()
    mhi[...], mlo[...] = split(mult[...])

    for q in range(chunks):
        arrived(None, panels.at[1 - p, chunk(q)], pan_r.at[(1 - p) * chunks + q])

    to_here = jnp.where(owner == m, place, -1).astype(F32)
    to_row = flat_row(to_here)
    landing = (iota((local_count, count), 0).astype(F32) == to_row).astype(F32)
    hit = jnp.sum(landing, axis=1, keepdims=True) > 0.0
    moved_in = select_rows(landing.astype(BF16), panels[...].reshape(count, columns))
    out[...] = jnp.where(hit, moved_in, rhs[...])

    def forward(h):
        for q in range(chunks):
            part, at = lpart(h, q, far), h * chunks + q
            sem = lc_r.at[far * 2 * chunks + at]
            arrived(m != 1, part, sem)
            send(m != 1, part, part, lc_f.at[at], sem, cols=side)

    forward(0)
    forward(1)
    for s in range(steps):
        r = 2 * s + 1 - p
        for n in range(parts):
            arrived(None, slice_of(r, n), c_r.at[r * parts + n])

    where_col = jnp.where(own_col >= 0.0, own_col * slots + slot_col, -1.0)
    pool = wide(comp[...])

    def panel_rows(k):
        target = where_col[k * blk:(k + 1) * blk]
        pick = (target == iota((blk, ranks * slots), 1).astype(F32)).astype(F32).astype(BF16)
        return jnp.where(target >= 0.0, fold(mm(pick, pool)), panels[k])

    def solve(k, values):
        first = dot_wide(split(inv[2 * k]), values[:hb])
        rest = values[hb:] - dot_wide(split(diag[k, hb:, :hb]), first)
        return jnp.concatenate([first, dot_wide(split(inv[2 * k + 1]), rest)], axis=0)

    y0 = solve(0, panel_rows(0))
    start = panel_rows(1)

    for owner in (side, corner):
        for h in range(2):
            for q in range(chunks):
                arrived(m != 1, lpart(h, q, owner), lc_r.at[(owner * 2 + h) * chunks + q])
    y1 = solve(1, start - dot_wide(split(lbuf[...]), y0))
    out[...] = out[...] - dot_wide((mhi[0], mlo[0]), y0) - dot_wide((mhi[1], mlo[1]), y1)

    @pl.when(m == 0)
    def _():
        out[:blk] = y0

    @pl.when(m == 1)
    def _():
        out[:blk] = y1

    for cond, copy in pending:
        when(cond, copy.wait_send)


def shards(ranks, groups, rhs, diag_blocks, multipliers, pivots):
    cycles, blk, columns = rhs.shape
    local_count = cycles * blk
    count = pivots.shape[0] * groups
    slots = 3 * count // (2 * ranks)
    chunks, parts = 4, 3
    dma = pltpu.SemaphoreType.DMA
    solved = pl.pallas_call(
        functools.partial(kernel, ranks, groups, blk, slots, chunks, parts),
        out_shape=jax.ShapeDtypeStruct((local_count, columns), F32),
        in_specs=[
            pl.BlockSpec(memory_space=pltpu.VMEM),
            pl.BlockSpec(memory_space=pl.ANY),
            pl.BlockSpec(memory_space=pl.ANY),
            pl.BlockSpec(memory_space=pltpu.VMEM),
        ],
        out_specs=pl.BlockSpec(memory_space=pltpu.VMEM),
        scratch_shapes=[
            pltpu.VMEM((2, blk, columns), F32),
            pltpu.VMEM((blk, blk), F32),
            pltpu.VMEM((ranks * slots, columns), F32),
            pltpu.VMEM((groups, pivots.shape[0] // 128, 128), jnp.int32),
            pltpu.VMEM((2, blk, blk), F32),
            pltpu.VMEM((2, local_count, blk), F32),
            pltpu.VMEM((4, blk // 2, blk // 2), F32),
            pltpu.VMEM((2, local_count, blk), BF16),
            pltpu.VMEM((2, local_count, blk), BF16),
            dma((3,)), dma((groups,)), dma((groups,)),
            dma((chunks,)), dma((chunks,)), dma((2 * chunks,)),
            dma((chunks,)), dma((2 * chunks,)), dma((2 * chunks,)),
            dma((4 * chunks,)), dma((2 * chunks,)), dma((2 * groups * chunks,)),
            dma((ranks * parts,)), dma((ranks * parts,)), dma((ranks * parts,)), dma((ranks * parts,)),
        ],
        compiler_params=pltpu.CompilerParams(
            collective_id=0, has_side_effects=True, vmem_limit_bytes=60 * 1024 * 1024
        ),
    )(
        rhs.reshape(local_count, columns),
        diag_blocks,
        multipliers.reshape(multipliers.shape[0], local_count, blk),
        pivots.reshape(-1, 128),
    )
    return solved.reshape(cycles, blk, columns)


def solution(mesh):
    placed = (P(None, "rows", "cols"), P(), P(None, None, "rows", None), P("cols"))
    return jax.shard_map(
        functools.partial(shards, mesh.shape["rows"], mesh.shape["cols"]),
        mesh=mesh, in_specs=placed, out_specs=P(None, "rows", "cols"), check_vma=False,
    )
```
